32 devices in a mesh: pairs: 2 (over y), aa: 4 (over z), ba: 4 (over x, core).
Axes of the slice: x: 2, y: 2, z: 4, core: 2. Of those that a mesh axis runs over, the one named last changes fastest.
Arguments:
- feats_a: float32 [1024, 256], P(('pairs', 'aa', 'ba')), parts along dimension 0, may hold values from -24 to 24
- feats_b: float32 [512, 256], P(('pairs', 'ba', 'aa')), parts along dimension 0, may hold values from -24 to 24
- qk_weight: float32 [2, 256, 256], replicated, may hold values from -0.375 to 0.375
- qk_bias: float32 [2, 256], replicated, may hold values from -3 to 3
- value_weight: float32 [2, 256, 256], replicated, may hold values from -0.375 to 0.375
- value_bias: float32 [2, 256], replicated, may hold values from -3 to 3
- out_weight: float32 [2, 256, 256], replicated, may hold values from -0.375 to 0.375
- out_bias: float32 [2, 256], replicated, may hold values from -3 to 3
- hidden_weight: float32 [2, 512, 512], replicated, may hold values from -0.25 to 0.25
- hidden_bias: float32 [2, 512], replicated, may hold values from -3 to 3
- norm_gain: float32 [2, 512], replicated, may hold values from 0.25 to 1.75
- norm_bias: float32 [2, 512], replicated, may hold values from -3 to 3
- final_weight: float32 [2, 512, 256], replicated, may hold values from -0.25 to 0.25
- final_bias: float32 [2, 256], replicated, may hold values from -3 to 3
Outputs:
- out_a: float32 [1024, 256], P(('pairs', 'aa', 'ba')), parts along dimension 0
- out_b: float32 [512, 256], P(('pairs', 'ba', 'aa')), parts along dimension 0
The draws below stay inside these ranges and needn't reach their ends.
There are 2 independent parts, one for each index of `pairs`. The reference program is written for one: setup_inputs(seed, part) draws one part's arguments, and reference() takes and returns one part's arrays. A program takes and returns all parts, laid end to end along the dimension named above; an argument that names none is the same for every part. Nothing has to cross between parts.
All inputs are finite; a program needn't handle non-finite values.
Results may differ from the reference program's by a relative error of at most 0.0003.
Values sent between devices are 32-bit elements; how exact they have to be, the bound alone decides.
No kernel may reach another device: no remote copies, remote signals or barrier semaphores. Data moves between devices by JAX's collectives and lax.ppermute only.
A program may use at most 64 MiB of HBM per device.

```python
import math
import jax
import jax.numpy as jnp
from jax import lax

D = 256
HEADS = 4
HEAD_SIZE = 64
WIDE = 512
LAYERS = 2
M = 512
N = 256


def draw_features(key, row_count, salt_value):
    values = jnp.clip(jax.random.normal(jax.random.fold_in(key, salt_value), (row_count, D), jnp.float32), -6.0, 6.0)
    return values


def draw_feats_a(key, part):
    return draw_features(key, M, 11)


def draw_feats_b(key, part):
    return draw_features(key, N, 31)


def scatter_about(rng, shape, scale, limit, held_as=jnp.bfloat16):
    entries = jax.random.normal(rng, shape, jnp.float32) * scale
    return jnp.minimum(jnp.maximum(entries, -limit), limit).astype(held_as)


def setup_inputs(seed: int = 0, part: int = 0) -> dict:
    arg_keys = jax.random.split(jax.random.key(seed), 15)
    own_keys = jax.random.split(jax.random.fold_in(arg_keys[14], part), 15)
    return {
        "feats_a": draw_feats_a(jax.random.fold_in(jax.random.fold_in(arg_keys[14], part), 71), part),
        "feats_b": draw_feats_b(jax.random.fold_in(jax.random.fold_in(arg_keys[14], part), 71), part),
        "qk_weight": scatter_about(arg_keys[2], (LAYERS, D, D), D ** -0.5, 0.375, jnp.float32),
        "qk_bias": scatter_about(arg_keys[3], (LAYERS, D), 0.5, 3.0, jnp.float32),
        "value_weight": scatter_about(arg_keys[4], (LAYERS, D, D), D ** -0.5, 0.375, jnp.float32),
        "value_bias": scatter_about(arg_keys[5], (LAYERS, D), 0.5, 3.0, jnp.float32),
        "out_weight": scatter_about(arg_keys[6], (LAYERS, D, D), D ** -0.5, 0.375, jnp.float32),
        "out_bias": scatter_about(arg_keys[7], (LAYERS, D), 0.5, 3.0, jnp.float32),
        "hidden_weight": scatter_about(arg_keys[8], (LAYERS, WIDE, WIDE), WIDE ** -0.5, 0.25, jnp.float32),
        "hidden_bias": scatter_about(arg_keys[9], (LAYERS, WIDE), 0.5, 3.0, jnp.float32),
        "norm_gain": jnp.clip(1.0 + 0.15 * jax.random.normal(arg_keys[10], (LAYERS, WIDE), jnp.float32), 0.25, 1.75),
        "norm_bias": scatter_about(arg_keys[11], (LAYERS, WIDE), 0.5, 3.0, jnp.float32),
        "final_weight": scatter_about(arg_keys[12], (LAYERS, WIDE, D), WIDE ** -0.5, 0.25, jnp.float32),
        "final_bias": scatter_about(arg_keys[13], (LAYERS, D), 0.5, 3.0, jnp.float32),
    }


EXACT_RESULT = lax.Precision.HIGHEST

def matmul(left, right):
    return jnp.dot(left, right, precision=EXACT_RESULT)

def layer_norm(values, gain, offset):
    average = lax.optimization_barrier(jnp.mean(values, -1, keepdims=True))
    centred = values - average
    spread = lax.optimization_barrier(jnp.mean(centred * centred, -1, keepdims=True))
    return centred / jnp.sqrt(spread + 1e-05) * gain + offset

def feed_forward(state, message, hidden_weight, hidden_bias, norm_gain, norm_bias, final_weight, final_bias):
    joined = jnp.concatenate([state, message], -1)
    hidden = matmul(joined, hidden_weight) + hidden_bias
    active = jax.nn.gelu(layer_norm(hidden, norm_gain, norm_bias), approximate=False)
    return state + matmul(active, final_weight) + final_bias

def cross_messages(query_first_image, value_a, query_second_image, value_b):
    block_rows = math.gcd(M, 1024)
    count = M // block_rows
    softmax_temper = HEAD_SIZE ** (-0.5)
    query_blocks = query_first_image.reshape(count, block_rows, HEADS, HEAD_SIZE)
    value_blocks = value_a.reshape(count, block_rows, HEADS, HEAD_SIZE)

    def advance(running, pieces):
        col_top, col_sum, numerator = running
        query_slice, value_piece = pieces
        score_matrix = jnp.einsum('cjg,xjg->jcx', query_slice, query_second_image, precision=EXACT_RESULT) * softmax_temper
        row_top = lax.optimization_barrier(jnp.max(score_matrix, 2, keepdims=True))
        row_exp = jnp.exp(score_matrix - row_top)
        row_sum = jnp.transpose(lax.optimization_barrier(jnp.sum(row_exp, 2)))
        row_msg = jnp.einsum('hab,bhd->ahd', row_exp, value_b, precision=EXACT_RESULT) / row_sum[:, :, None]
        new_top = jnp.maximum(col_top, lax.optimization_barrier(jnp.max(score_matrix, 1)))
        col_exp = jnp.exp(score_matrix - new_top[:, None, :])
        rescale = jnp.exp(col_top - new_top)
        col_sum = col_sum * rescale + lax.optimization_barrier(jnp.sum(col_exp, 1))
        numerator = numerator * rescale[:, :, None] + jnp.einsum('hab,ahd->hbd', col_exp, value_piece, precision=EXACT_RESULT)
        return ((new_top, col_sum, numerator), row_msg)
    start = (jnp.full((HEADS, N), -jnp.inf, jnp.float32), jnp.zeros((HEADS, N), jnp.float32), jnp.zeros((HEADS, N, HEAD_SIZE), jnp.float32))
    running, row_blocks = lax.scan(advance, start, (query_blocks, value_blocks))
    msg_a = row_blocks.reshape(M, D)
    msg_b = jnp.transpose(running[2] / running[1][:, :, None], (1, 0, 2)).reshape(N, D)
    return (msg_a, msg_b)

def reference(feats_a, feats_b, qk_weight, qk_bias, value_weight, value_bias, out_weight, out_bias, hidden_weight, hidden_bias, norm_gain, norm_bias, final_weight, final_bias):
    first = feats_a
    second = feats_b
    for layer_index in range(LAYERS):
        query_first_image = (matmul(first, qk_weight[layer_index]) + qk_bias[layer_index]).reshape(M, HEADS, HEAD_SIZE)
        value_a = (matmul(first, value_weight[layer_index]) + value_bias[layer_index]).reshape(M, HEADS, HEAD_SIZE)
        query_second_image = (matmul(second, qk_weight[layer_index]) + qk_bias[layer_index]).reshape(N, HEADS, HEAD_SIZE)
        value_b = (matmul(second, value_weight[layer_index]) + value_bias[layer_index]).reshape(N, HEADS, HEAD_SIZE)
        msg_a, msg_b = cross_messages(query_first_image, value_a, query_second_image, value_b)
        reply_a = matmul(msg_a, out_weight[layer_index]) + out_bias[layer_index]
        reply_b = matmul(msg_b, out_weight[layer_index]) + out_bias[layer_index]
        first = feed_forward(first, reply_a, hidden_weight[layer_index], hidden_bias[layer_index], norm_gain[layer_index], norm_bias[layer_index], final_weight[layer_index], final_bias[layer_index])
        second = feed_forward(second, reply_b, hidden_weight[layer_index], hidden_bias[layer_index], norm_gain[layer_index], norm_bias[layer_index], final_weight[layer_index], final_bias[layer_index])
    return (first, second)
```

```python
import functools

import jax
import jax.numpy as jnp
from jax import lax
from jax.experimental import pallas as pl
from jax.experimental.pallas import tpu as pltpu
from jax.sharding import PartitionSpec as P

HEADS = 4
EPS = 1e-05
EXACT_RESULT = lax.Precision.HIGHEST
GATHER_BYTES = 2 << 20


def split(x):
    hi = x.astype(jnp.bfloat16)
    return hi, (x - hi.astype(jnp.float32)).astype(jnp.bfloat16)


def dot(a, b, transposed=False):
    contract = ((1,), (1 if transposed else 0,))
    return lax.dot_general(a, b, (contract, ((), ())), preferred_element_type=jnp.float32)


def dot3(a, b, transposed=False):
    return dot(a[0], b[0], transposed) + (dot(a[0], b[1], transposed) + dot(a[1], b[0], transposed))


def head_masks(rows, width, heads):
    lane = lax.broadcasted_iota(jnp.int32, (rows, width), 1)
    size = width // heads
    return [(lane >= h * size) & (lane < (h + 1) * size) for h in range(heads)]


def attend(query, key, value, heads):
    rows, width = query.shape
    masks = head_masks(rows, width, heads)
    stacked = jnp.concatenate([jnp.where(m, query, 0.0) for m in masks], 0)
    scores = dot3(split(stacked), key, True)
    top = jnp.max(scores, 1, keepdims=True)
    weights = jnp.exp(scores - top)
    total = jnp.sum(weights, 1, keepdims=True)
    numer = dot3(split(weights), value)
    ratio = numer * (1.0 / total)
    out = jnp.zeros((rows, width), jnp.float32)
    for h, m in enumerate(masks):
        out = jnp.where(m, ratio[h * rows : (h + 1) * rows], out)
    return out


def feed_forward(x, msg, w):
    y = dot3(split(msg), w["out"]) + w["out_b"]
    width = x.shape[1]
    hidden = dot3(split(x), w["hid_x"]) + dot3(split(y), w["hid_y"]) + w["hid_b"]
    centred = hidden - jnp.mean(hidden, 1, keepdims=True)
    spread = jnp.mean(centred * centred, 1, keepdims=True)
    normed = centred * lax.rsqrt(spread + EPS) * w["gain"] + w["shift"]
    active = 0.5 * normed * (1.0 + lax.erf(normed * (0.5**0.5)))
    return x + dot3(split(active), w["fin"]) + w["fin_b"]


def load_weights(refs):
    qk, qk_b, val, val_b, out, out_b, hid, hid_b, gain, shift, fin, fin_b = refs
    width = qk.shape[0]
    return dict(
        qk=split(qk[...]),
        qk_b=qk_b[...],
        val=split(val[...]),
        val_b=val_b[...],
        out=split(out[...]),
        out_b=out_b[...],
        hid_x=split(hid[:width, :]),
        hid_y=split(hid[width:, :]),
        hid_b=hid_b[...],
        gain=gain[...],
        shift=shift[...],
        fin=split(fin[...]),
        fin_b=fin_b[...],
    )


def layer_kernel(n_src, n_tgt, rows_a, rows_b, heads, final, *refs):
    srcs = refs[:n_src]
    w = load_weights(refs[n_src : n_src + 12])
    outs = refs[n_src + 12 :]
    xs = jnp.concatenate([s[:rows_a, :] for s in srcs] + [s[rows_a:, :] for s in srcs], 0)
    halves = split(xs)
    width = xs.shape[1]
    qk = dot3(halves, w["qk"]) + w["qk_b"]
    val = dot3(halves, w["val"]) + w["val_b"]
    count_a = n_src * rows_a
    temper = (width // heads) ** (-0.5)
    key = split(qk)
    value = split(val)
    tgt_a, tgt_b = n_tgt * rows_a, n_tgt * rows_b
    key_a, key_b = tuple(k[:count_a] for k in key), tuple(k[count_a:] for k in key)
    value_a, value_b = tuple(v[:count_a] for v in value), tuple(v[count_a:] for v in value)
    msg_a = attend(qk[:tgt_a] * temper, key_b, value_b, heads)
    msg_b = attend(qk[count_a : count_a + tgt_b] * temper, key_a, value_a, heads)
    x = jnp.concatenate([xs[:tgt_a], xs[count_a : count_a + tgt_b]], 0)
    res = feed_forward(x, jnp.concatenate([msg_a, msg_b], 0), w)
    if final:
        outs[0][...] = res[:tgt_a]
        outs[1][...] = res[tgt_a:]
    else:
        for j in range(n_tgt):
            outs[j][:rows_a, :] = res[j * rows_a : (j + 1) * rows_a]
            outs[j][rows_a:, :] = res[tgt_a + j * rows_b : tgt_a + (j + 1) * rows_b]


def layer_call(blocks, n_tgt, rows_a, rows_b, weights, layer, final):
    rows, width = blocks[0].shape
    ws = [w if w.ndim == 3 else w[:, None, :] for w in weights]
    in_specs = [pl.BlockSpec(b.shape, lambda i: (0, 0)) for b in blocks] + [
        pl.BlockSpec((None,) + w.shape[1:], lambda i: (layer, 0, 0)) for w in ws
    ]
    if final:
        shapes = [(n_tgt * rows_a, width), (n_tgt * rows_b, width)]
    else:
        shapes = [(rows, width)] * n_tgt
    return pl.pallas_call(
        functools.partial(layer_kernel, len(blocks), n_tgt, rows_a, rows_b, HEADS, final),
        grid=(1,),
        in_specs=in_specs,
        out_specs=[pl.BlockSpec(s, lambda i: (0, 0)) for s in shapes],
        out_shape=[jax.ShapeDtypeStruct(s, jnp.float32) for s in shapes],
        compiler_params=pltpu.CompilerParams(vmem_limit_bytes=48 << 20),
        name=f"layer{layer}",
    )(*blocks, *ws)


def hop(x, sizes, step_a, step_b):
    size_a, size_b = sizes
    pairs = [
        (a * size_b + b, (a ^ step_a) * size_b + (b ^ step_b)) for a in range(size_a) for b in range(size_b)
    ]
    return lax.ppermute(x, ("aa", "ba"), pairs)


def replicated(sizes, feats_a, feats_b, *weights):
    size_a, size_b = sizes
    rows_a, rows_b = feats_a.shape[0], feats_b.shape[0]
    own = jnp.concatenate([feats_a, feats_b], 0)
    blocks = [own] + [hop(own, sizes, k, 0) for k in range(1, size_a)]
    step = size_b // 2
    while step > 1:
        blocks = blocks + [hop(b, sizes, 0, step) for b in blocks]
        step //= 2
    others = [hop(b, sizes, 0, 1) for b in blocks] if size_b > 1 else []
    layers = weights[0].shape[0]
    for layer in range(layers - 1):
        blocks = list(layer_call(blocks + others, len(blocks), rows_a, rows_b, weights, layer, False))
        others = [hop(b, sizes, 0, 1) for b in blocks] if size_b > 1 else []
    return tuple(layer_call(blocks + others, 1, rows_a, rows_b, weights, layers - 1, True))


def matmul(left, right):
    return jnp.dot(left, right, precision=EXACT_RESULT)


def layer_norm(values, gain, offset):
    average = jnp.mean(values, -1, keepdims=True)
    centred = values - average
    spread = jnp.mean(centred * centred, -1, keepdims=True)
    return centred / jnp.sqrt(spread + EPS) * gain + offset


def feed_forward_rows(state, message, hidden_weight, hidden_bias, norm_gain, norm_bias, final_weight, final_bias):
    joined = jnp.concatenate([state, message], -1)
    hidden = matmul(joined, hidden_weight) + hidden_bias
    active = jax.nn.gelu(layer_norm(hidden, norm_gain, norm_bias), approximate=False)
    return state + matmul(active, final_weight) + final_bias


def settle_owner(numer, tops, totals):
    best = jnp.max(tops, 0)
    weight = jnp.exp(tops - best[None])
    denom = jnp.sum(weight * totals, 0)
    sources = numer.shape[0]
    rows = numer.shape[1]
    heads = tops.shape[2]
    shaped = numer.reshape(sources, rows, heads, -1)
    joined = jnp.sum(shaped * weight[:, :, :, None], 0) / denom[:, :, None]
    return joined.reshape(rows, -1)


def partitioned(
    feats_a,
    feats_b,
    qk_weight,
    qk_bias,
    value_weight,
    value_bias,
    out_weight,
    out_bias,
    hidden_weight,
    hidden_bias,
    norm_gain,
    norm_bias,
    final_weight,
    final_bias,
):
    width = feats_a.shape[1]
    head_count = HEADS
    head_width = width // head_count
    softmax_temper = head_width ** (-0.5)
    first = feats_a
    second = feats_b

    def exchange(x, axis):
        return lax.all_to_all(x[None], axis, split_axis=1, concat_axis=0, tiled=True)

    for layer in range(qk_weight.shape[0]):
        joint_weight = jnp.concatenate([qk_weight[layer], value_weight[layer]], 1)
        joint_bias = jnp.concatenate([qk_bias[layer], value_bias[layer]], 0)
        proj_a = matmul(first, joint_weight) + joint_bias
        proj_b = matmul(second, joint_weight) + joint_bias
        block_a = lax.all_gather(proj_a, "ba", axis=0, tiled=True)
        block_b = lax.all_gather(proj_b, "aa", axis=0, tiled=True)
        query_a = block_a[:, :width].reshape(-1, head_count, head_width)
        value_a = block_a[:, width:].reshape(-1, head_count, head_width)
        query_b = block_b[:, :width].reshape(-1, head_count, head_width)
        value_b = block_b[:, width:].reshape(-1, head_count, head_width)
        scores = jnp.einsum("cjg,xjg->jcx", query_a, query_b, precision=EXACT_RESULT) * softmax_temper
        row_local = jnp.max(scores, 2)
        col_local = jnp.max(scores, 1)
        row_exp = jnp.exp(scores - row_local[:, :, None])
        col_exp = jnp.exp(scores - col_local[:, None, :])
        numer_a = jnp.einsum("hab,bhd->ahd", row_exp, value_b, precision=EXACT_RESULT).reshape(-1, width)
        numer_b = jnp.einsum("hab,ahd->bhd", col_exp, value_a, precision=EXACT_RESULT).reshape(-1, width)
        msg_a = settle_owner(
            exchange(numer_a, "ba"),
            exchange(jnp.transpose(row_local), "ba"),
            exchange(jnp.transpose(jnp.sum(row_exp, 2)), "ba"),
        )
        msg_b = settle_owner(
            exchange(numer_b, "aa"),
            exchange(jnp.transpose(col_local), "aa"),
            exchange(jnp.transpose(jnp.sum(col_exp, 1)), "aa"),
        )
        tail = (
            hidden_weight[layer],
            hidden_bias[layer],
            norm_gain[layer],
            norm_bias[layer],
            final_weight[layer],
            final_bias[layer],
        )
        first = feed_forward_rows(first, matmul(msg_a, out_weight[layer]) + out_bias[layer], *tail)
        second = feed_forward_rows(second, matmul(msg_b, out_weight[layer]) + out_bias[layer], *tail)
    return (first, second)


def shards(sizes, feats_a, feats_b, *weights):
    devices = sizes[0] * sizes[1]
    gathered = devices * (feats_a.size + feats_b.size) * feats_a.dtype.itemsize
    regular = all(n & (n - 1) == 0 for n in sizes) and feats_a.shape[0] % 8 == 0 and feats_b.shape[0] % 8 == 0
    if regular and gathered <= GATHER_BYTES:
        return replicated(sizes, feats_a, feats_b, *weights)
    return partitioned(feats_a, feats_b, *weights)


def solution(mesh):
    sizes = (mesh.shape["aa"], mesh.shape["ba"])
    in_specs = (P(("pairs", "aa", "ba"), None), P(("pairs", "ba", "aa"), None)) + (P(),) * 12
    out_specs = (P(("pairs", "aa", "ba"), None), P(("pairs", "ba", "aa"), None))
    return jax.shard_map(
        functools.partial(shards, sizes), mesh=mesh, in_specs=in_specs, out_specs=out_specs, check_vma=False
    )
```

```python
import functools

import jax
import jax.numpy as jnp
from jax import lax
from jax.experimental import pallas as pl
from jax.experimental.pallas import tpu as pltpu
from jax.sharding import PartitionSpec as P

HEADS = 4
EPS = 1e-05
EXACT_RESULT = lax.Precision.HIGHEST
GATHER_BYTES = 2 << 20


def split(x):
    hi = x.astype(jnp.bfloat16)
    return hi, (x - hi.astype(jnp.float32)).astype(jnp.bfloat16)


def dot(a, b, transposed=False):
    contract = ((1,), (1 if transposed else 0,))
    return lax.dot_general(a, b, (contract, ((), ())), preferred_element_type=jnp.float32)


def dot3(a, b, transposed=False):
    return dot(a[0], b[0], transposed) + (dot(a[0], b[1], transposed) + dot(a[1], b[0], transposed))


def head_masks(rows, width, heads):
    lane = lax.broadcasted_iota(jnp.int32, (rows, width), 1)
    size = width // heads
    return [(lane >= h * size) & (lane < (h + 1) * size) for h in range(heads)]


def attend(query, key, value, heads):
    rows, width = query.shape
    masks = head_masks(rows, width, heads)
    stacked = jnp.concatenate([jnp.where(m, query, 0.0) for m in masks], 0)
    scores = dot3(split(stacked), key, True)
    top = jnp.max(scores, 1, keepdims=True)
    weights = jnp.exp(scores - top)
    total = jnp.sum(weights, 1, keepdims=True)
    numer = dot3(split(weights), value)
    ratio = numer * (1.0 / total)
    out = jnp.zeros((rows, width), jnp.float32)
    for h, m in enumerate(masks):
        out = jnp.where(m, ratio[h * rows : (h + 1) * rows], out)
    return out


def anchor_kernel(x_ref, o_ref):
    del x_ref, o_ref


def anchor(x):
    vmem = pl.BlockSpec(memory_space=pltpu.VMEM)
    return pl.pallas_call(
        anchor_kernel,
        in_specs=[vmem],
        out_specs=vmem,
        out_shape=jax.ShapeDtypeStruct(x.shape, x.dtype),
        input_output_aliases={0: 0},
        cost_estimate=pl.CostEstimate(flops=10**10, bytes_accessed=1, transcendentals=0),
        compiler_params=pltpu.CompilerParams(vmem_limit_bytes=1 << 20),
        name="anchor",
    )(x)


def own_block(feats_a, feats_b):
    rows_a, rows_b = feats_a.shape[0], feats_b.shape[0]
    low = jnp.float32(-jnp.inf)
    padded_a = lax.pad(feats_a, low, [(0, rows_b, 0), (0, 0, 0)])
    padded_b = lax.pad(feats_b, low, [(rows_a, 0, 0), (0, 0, 0)])
    return jnp.maximum(padded_a, padded_b)


def layer_kernel(layer, spans, n_tgt, rows_a, rows_b, heads, final, *refs):
    srcs = refs[: len(spans)]
    rest = refs[len(spans) :]
    rows = rows_a + rows_b

    def mat(i):
        return split(rest[i][layer])

    def vec(i):
        return rest[5 + i][layer : layer + 1, :]

    qk_b, val_b, out_b, hid_b, gain, shift, fin_b = (vec(i) for i in range(7))
    outs = rest[12:]
    parts_a, parts_b = [], []
    for s, span in zip(srcs, spans):
        for j in range(span):
            parts_a.append(s[j * rows : j * rows + rows_a, :])
            parts_b.append(s[j * rows + rows_a : (j + 1) * rows, :])
    xs = jnp.concatenate(parts_a + parts_b, 0)
    halves = split(xs)
    width = xs.shape[1]
    qk = dot3(halves, mat(0)) + qk_b
    val = dot3(halves, mat(1)) + val_b
    count_a = len(parts_a) * rows_a
    temper = (width // heads) ** (-0.5)
    key = split(qk)
    value = split(val)
    tgt_a, tgt_b = n_tgt * rows_a, n_tgt * rows_b
    key_a, key_b = tuple(k[:count_a] for k in key), tuple(k[count_a:] for k in key)
    value_a, value_b = tuple(v[:count_a] for v in value), tuple(v[count_a:] for v in value)
    msg_a = attend(qk[:tgt_a] * temper, key_b, value_b, heads)
    msg_b = attend(qk[count_a : count_a + tgt_b] * temper, key_a, value_a, heads)
    x = jnp.concatenate([xs[:tgt_a], xs[count_a : count_a + tgt_b]], 0)
    msg = jnp.concatenate([msg_a, msg_b], 0)
    y = dot3(split(msg), mat(2)) + out_b
    hid = mat(3)
    hid_x, hid_y = tuple(h[:width] for h in hid), tuple(h[width:] for h in hid)
    hidden = dot3(split(x), hid_x) + dot3(split(y), hid_y) + hid_b
    centred = hidden - jnp.mean(hidden, 1, keepdims=True)
    spread = jnp.mean(centred * centred, 1, keepdims=True)
    normed = centred * lax.rsqrt(spread + EPS) * gain + shift
    active = 0.5 * normed * (1.0 + lax.erf(normed * (0.5**0.5)))
    res = x + dot3(split(active), mat(4)) + fin_b
    if final:
        outs[0][...] = res[:tgt_a]
        outs[1][...] = res[tgt_a:]
    else:
        for j in range(n_tgt):
            outs[0][j * rows : j * rows + rows_a, :] = res[j * rows_a : (j + 1) * rows_a]
            outs[0][j * rows + rows_a : (j + 1) * rows, :] = res[tgt_a + j * rows_b : tgt_a + (j + 1) * rows_b]


def layer_call(arrays, n_tgt, rows_a, rows_b, weights, layer, final):
    rows = rows_a + rows_b
    width = arrays[0].shape[1]
    spans = tuple(a.shape[0] // rows for a in arrays)
    vmem = pl.BlockSpec(memory_space=pltpu.VMEM)
    shapes = [(n_tgt * rows_a, width), (n_tgt * rows_b, width)] if final else [(n_tgt * rows, width)]
    ws = [w for group in weights for w in group]
    return pl.pallas_call(
        functools.partial(layer_kernel, layer, spans, n_tgt, rows_a, rows_b, HEADS, final),
        in_specs=[vmem] * (len(arrays) + len(ws)),
        out_specs=[vmem] * len(shapes),
        out_shape=[jax.ShapeDtypeStruct(s, jnp.float32) for s in shapes],
        compiler_params=pltpu.CompilerParams(vmem_limit_bytes=24 << 20),
        name=f"layer{layer}",
    )(*arrays, *ws)


def hop(x, sizes, step_a, step_b):
    size_a, size_b = sizes
    pairs = [
        (a * size_b + b, (a ^ step_a) * size_b + (b ^ step_b)) for a in range(size_a) for b in range(size_b)
    ]
    return lax.ppermute(x, ("aa", "ba"), pairs)


def replicated(sizes, feats_a, feats_b, *weights):
    size_a, size_b = sizes
    rows_a, rows_b = feats_a.shape[0], feats_b.shape[0]
    qk, qk_b, val, val_b, out, out_b, hid, hid_b, gain, shift, fin, fin_b = weights
    own = anchor(own_block(feats_a, feats_b))
    blocks = [own] + [hop(own, sizes, k, 0) for k in range(1, size_a)]
    step = size_b // 2
    while step > 1:
        blocks = blocks + [hop(b, sizes, 0, step) for b in blocks]
        step //= 2
    ready = ((qk, val, out, hid, fin), (qk_b, val_b, out_b, hid_b, gain, shift, fin_b))
    half = len(blocks)
    arrays = blocks + ([hop(b, sizes, 0, 1) for b in blocks] if size_b > 1 else [])
    layers = qk.shape[0]
    for layer in range(layers - 1):
        (result,) = layer_call(arrays, half, rows_a, rows_b, ready, layer, False)
        arrays = [result] + ([hop(result, sizes, 0, 1)] if size_b > 1 else [])
    return tuple(layer_call(arrays, 1, rows_a, rows_b, ready, layers - 1, True))


def matmul(left, right):
    return jnp.dot(left, right, precision=EXACT_RESULT)


def layer_norm(values, gain, offset):
    average = jnp.mean(values, -1, keepdims=True)
    centred = values - average
    spread = jnp.mean(centred * centred, -1, keepdims=True)
    return centred / jnp.sqrt(spread + EPS) * gain + offset


def feed_forward_rows(state, message, hidden_weight, hidden_bias, norm_gain, norm_bias, final_weight, final_bias):
    joined = jnp.concatenate([state, message], -1)
    hidden = matmul(joined, hidden_weight) + hidden_bias
    active = jax.nn.gelu(layer_norm(hidden, norm_gain, norm_bias), approximate=False)
    return state + matmul(active, final_weight) + final_bias


def settle_owner(numer, tops, totals):
    best = jnp.max(tops, 0)
    weight = jnp.exp(tops - best[None])
    denom = jnp.sum(weight * totals, 0)
    sources = numer.shape[0]
    rows = numer.shape[1]
    heads = tops.shape[2]
    shaped = numer.reshape(sources, rows, heads, -1)
    joined = jnp.sum(shaped * weight[:, :, :, None], 0) / denom[:, :, None]
    return joined.reshape(rows, -1)


def partitioned(
    feats_a,
    feats_b,
    qk_weight,
    qk_bias,
    value_weight,
    value_bias,
    out_weight,
    out_bias,
    hidden_weight,
    hidden_bias,
    norm_gain,
    norm_bias,
    final_weight,
    final_bias,
):
    width = feats_a.shape[1]
    head_count = HEADS
    head_width = width // head_count
    softmax_temper = head_width ** (-0.5)
    first = feats_a
    second = feats_b

    def exchange(x, axis):
        return lax.all_to_all(x[None], axis, split_axis=1, concat_axis=0, tiled=True)

    for layer in range(qk_weight.shape[0]):
        joint_weight = jnp.concatenate([qk_weight[layer], value_weight[layer]], 1)
        joint_bias = jnp.concatenate([qk_bias[layer], value_bias[layer]], 0)
        proj_a = matmul(first, joint_weight) + joint_bias
        proj_b = matmul(second, joint_weight) + joint_bias
        block_a = lax.all_gather(proj_a, "ba", axis=0, tiled=True)
        block_b = lax.all_gather(proj_b, "aa", axis=0, tiled=True)
        query_a = block_a[:, :width].reshape(-1, head_count, head_width)
        value_a = block_a[:, width:].reshape(-1, head_count, head_width)
        query_b = block_b[:, :width].reshape(-1, head_count, head_width)
        value_b = block_b[:, width:].reshape(-1, head_count, head_width)
        scores = jnp.einsum("cjg,xjg->jcx", query_a, query_b, precision=EXACT_RESULT) * softmax_temper
        row_local = jnp.max(scores, 2)
        col_local = jnp.max(scores, 1)
        row_exp = jnp.exp(scores - row_local[:, :, None])
        col_exp = jnp.exp(scores - col_local[:, None, :])
        numer_a = jnp.einsum("hab,bhd->ahd", row_exp, value_b, precision=EXACT_RESULT).reshape(-1, width)
        numer_b = jnp.einsum("hab,ahd->bhd", col_exp, value_a, precision=EXACT_RESULT).reshape(-1, width)
        msg_a = settle_owner(
            exchange(numer_a, "ba"),
            exchange(jnp.transpose(row_local), "ba"),
            exchange(jnp.transpose(jnp.sum(row_exp, 2)), "ba"),
        )
        msg_b = settle_owner(
            exchange(numer_b, "aa"),
            exchange(jnp.transpose(col_local), "aa"),
            exchange(jnp.transpose(jnp.sum(col_exp, 1)), "aa"),
        )
        tail = (
            hidden_weight[layer],
            hidden_bias[layer],
            norm_gain[layer],
            norm_bias[layer],
            final_weight[layer],
            final_bias[layer],
        )
        first = feed_forward_rows(first, matmul(msg_a, out_weight[layer]) + out_bias[layer], *tail)
        second = feed_forward_rows(second, matmul(msg_b, out_weight[layer]) + out_bias[layer], *tail)
    return (first, second)


def shards(sizes, feats_a, feats_b, *weights):
    devices = sizes[0] * sizes[1]
    gathered = devices * (feats_a.size + feats_b.size) * feats_a.dtype.itemsize
    regular = all(n & (n - 1) == 0 for n in sizes) and feats_a.shape[0] % 8 == 0 and feats_b.shape[0] % 8 == 0
    if regular and gathered <= GATHER_BYTES:
        return replicated(sizes, feats_a, feats_b, *weights)
    return partitioned(feats_a, feats_b, *weights)


def solution(mesh):
    sizes = (mesh.shape["aa"], mesh.shape["ba"])
    in_specs = (P(("pairs", "aa", "ba"), None), P(("pairs", "ba", "aa"), None)) + (P(),) * 12
    out_specs = (P(("pairs", "aa", "ba"), None), P(("pairs", "ba", "aa"), None))
    return jax.shard_map(
        functools.partial(shards, sizes), mesh=mesh, in_specs=in_specs, out_specs=out_specs, check_vma=False
    )
```

```python
import functools

import jax
import jax.numpy as jnp
from jax import lax
from jax.experimental import pallas as pl
from jax.experimental.pallas import tpu as pltpu
from jax.sharding import PartitionSpec as P

HEADS = 4
EPS = 1e-05
EXACT_RESULT = lax.Precision.HIGHEST
GATHER_BYTES = 2 << 20

GROUPS = 1


def split(x):
    hi = x.astype(jnp.bfloat16)
    return hi, (x - hi.astype(jnp.float32)).astype(jnp.bfloat16)


def dot(a, b, transposed=False):
    contract = ((1,), (1 if transposed else 0,))
    return lax.dot_general(a, b, (contract, ((), ())), preferred_element_type=jnp.float32)


def dot3(a, b, transposed=False):
    return dot(a[0], b[0], transposed) + (dot(a[0], b[1], transposed) + dot(a[1], b[0], transposed))


def turned(x):
    lanes = 128
    tiles = [pltpu.roll(x[:, t : t + lanes], lanes // 2, 1) for t in range(0, x.shape[1], lanes)]
    return jnp.concatenate(tiles, 1)


def lower_lanes(rows, dtype):
    del dtype
    return lax.broadcasted_iota(jnp.int32, (rows, 128), 1) < 64


def tile(x, h):
    t = (h // 2) * 128
    return x[:, t : t + 128]


def pair(x, x_turned, h):
    low = lower_lanes(x.shape[0], x.dtype)
    plain, flipped = tile(x, h), tile(x_turned, h)
    return split(jnp.where(low, plain, flipped) if h % 2 == 0 else jnp.where(low, flipped, plain))


def queries(x, x_turned, h):
    hi, lo = pair(x, x_turned, h)
    return jnp.concatenate([hi, lo], 1)


def mixed(x, x_turned, h):
    low = lower_lanes(x.shape[0], x.dtype)
    plain, flipped = tile(x, h), tile(x_turned, h)
    both = jnp.where(low, plain, flipped) if h % 2 == 0 else jnp.where(low, flipped, plain)
    hi = both.astype(jnp.bfloat16).astype(jnp.float32)
    return jnp.where(low, hi, both - hi).astype(jnp.bfloat16)


def attend(query, keys, values):
    results = []
    for q, k, v in zip(query, keys, values):
        scores = dot(q, k, True)
        weights = jnp.exp(scores - jnp.max(scores, 1, keepdims=True))
        hi, lo = split(weights)
        numer = dot(hi, v) + dot(lo, v)
        folded = numer[:, :128]
        folded = folded + pltpu.roll(folded, 64, 1)
        results.append(folded * (1.0 / numer[:, 128:]))
    low = lower_lanes(results[0].shape[0], jnp.float32)
    return jnp.concatenate([jnp.where(low, results[h], results[h + 1]) for h in range(0, len(results), 2)], 1)


def anchor_kernel(x_ref, o_ref):
    del x_ref, o_ref


def anchor(x):
    vmem = pl.BlockSpec(memory_space=pltpu.VMEM)
    return pl.pallas_call(
        anchor_kernel,
        in_specs=[vmem],
        out_specs=vmem,
        out_shape=jax.ShapeDtypeStruct(x.shape, x.dtype),
        input_output_aliases={0: 0},
        cost_estimate=pl.CostEstimate(flops=10**10, bytes_accessed=1, transcendentals=0),
        compiler_params=pltpu.CompilerParams(vmem_limit_bytes=1 << 20),
        name="anchor",
    )(x)


def own_block(feats_a, feats_b):
    rows_a, rows_b = feats_a.shape[0], feats_b.shape[0]
    low = jnp.float32(-jnp.inf)
    padded_a = lax.pad(feats_a, low, [(0, rows_b, 0), (0, 0, 0)])
    padded_b = lax.pad(feats_b, low, [(rows_a, 0, 0), (0, 0, 0)])
    return jnp.maximum(padded_a, padded_b)


def layer_kernel(layer, spans, n_tgt, rows_a, rows_b, heads, final, *refs):
    srcs = refs[: len(spans)]
    rest = refs[len(spans) :]
    rows = rows_a + rows_b

    def mat(i):
        return split(rest[i][layer])

    def vec(i):
        return rest[5 + i][layer : layer + 1, :]

    qk_b, val_b, out_b, hid_b, gain, shift, fin_b = (vec(i) for i in range(7))
    outs = rest[12:]
    parts_a, parts_b = [], []
    for s, span in zip(srcs, spans):
        for j in range(span):
            parts_a.append(s[j * rows : j * rows + rows_a, :])
            parts_b.append(s[j * rows + rows_a : (j + 1) * rows, :])
    xs = jnp.concatenate(parts_a + parts_b, 0)
    width = xs.shape[1]
    temper = (width // heads) ** (-0.5)
    halves = split(xs)
    qk = dot3(halves, mat(0)) + qk_b
    val = dot3(halves, mat(1)) + val_b
    count_a = len(parts_a) * rows_a
    tgt_a, tgt_b = n_tgt * rows_a, n_tgt * rows_b
    qk_t, val_t = turned(qk), turned(val)
    keys = [jnp.concatenate([m, m], 1) for m in (mixed(qk, qk_t, h) for h in range(heads))]
    ones = jnp.ones((xs.shape[0], 128), jnp.bfloat16)
    values = [jnp.concatenate([mixed(val, val_t, h), ones], 1) for h in range(heads)]
    rows_of = {0: slice(0, count_a), 1: slice(count_a, None)}
    out_w, hid, fin = mat(2), mat(3), mat(4)
    hid_x, hid_y = tuple(h[:width] for h in hid), tuple(h[width:] for h in hid)

    def finish(x, msg):
        y = dot3(split(msg), out_w) + out_b
        hidden = dot3(split(x), hid_x) + dot3(split(y), hid_y) + hid_b
        centred = hidden - jnp.mean(hidden, 1, keepdims=True)
        spread = jnp.mean(centred * centred, 1, keepdims=True)
        normed = centred * lax.rsqrt(spread + EPS) * gain + shift
        active = 0.5 * normed * (1.0 + lax.erf(normed * (0.5**0.5)))
        return x + dot3(split(active), fin) + fin_b

    def messages(start, stop, side):
        q, q_t = qk[start:stop] * temper, qk_t[start:stop] * temper
        other = rows_of[1 - side]
        return attend([queries(q, q_t, h) for h in range(heads)], [k[other] for k in keys], [v[other] for v in values])

    res = []
    for g in range(GROUPS if n_tgt % GROUPS == 0 else 1):
        groups = GROUPS if n_tgt % GROUPS == 0 else 1
        a0, a1 = g * tgt_a // groups, (g + 1) * tgt_a // groups
        b0, b1 = count_a + g * tgt_b // groups, count_a + (g + 1) * tgt_b // groups
        msg = jnp.concatenate([messages(a0, a1, 0), messages(b0, b1, 1)], 0)
        res.append((finish(jnp.concatenate([xs[a0:a1], xs[b0:b1]], 0), msg), a1 - a0))
    res = jnp.concatenate([r[:n] for r, n in res] + [r[n:] for r, n in res], 0)
    if final:
        outs[0][...] = res[:tgt_a]
        outs[1][...] = res[tgt_a:]
    else:
        for j in range(n_tgt):
            outs[0][j * rows : j * rows + rows_a, :] = res[j * rows_a : (j + 1) * rows_a]
            outs[0][j * rows + rows_a : (j + 1) * rows, :] = res[tgt_a + j * rows_b : tgt_a + (j + 1) * rows_b]


def layer_call(arrays, n_tgt, rows_a, rows_b, weights, layer, final):
    rows = rows_a + rows_b
    width = arrays[0].shape[1]
    spans = tuple(a.shape[0] // rows for a in arrays)
    vmem = pl.BlockSpec(memory_space=pltpu.VMEM)
    shapes = [(n_tgt * rows_a, width), (n_tgt * rows_b, width)] if final else [(n_tgt * rows, width)]
    ws = [w for group in weights for w in group]
    return pl.pallas_call(
        functools.partial(layer_kernel, layer, spans, n_tgt, rows_a, rows_b, HEADS, final),
        in_specs=[vmem] * (len(arrays) + len(ws)),
        out_specs=[vmem] * len(shapes),
        out_shape=[jax.ShapeDtypeStruct(s, jnp.float32) for s in shapes],
        compiler_params=pltpu.CompilerParams(vmem_limit_bytes=24 << 20),
        name=f"layer{layer}",
    )(*arrays, *ws)


def hop(x, sizes, step_a, step_b):
    size_a, size_b = sizes
    pairs = [
        (a * size_b + b, (a ^ step_a) * size_b + (b ^ step_b)) for a in range(size_a) for b in range(size_b)
    ]
    return lax.ppermute(x, ("aa", "ba"), pairs)


def replicated(sizes, feats_a, feats_b, *weights):
    size_a, size_b = sizes
    rows_a, rows_b = feats_a.shape[0], feats_b.shape[0]
    qk, qk_b, val, val_b, out, out_b, hid, hid_b, gain, shift, fin, fin_b = weights
    own = anchor(own_block(feats_a, feats_b))
    blocks = [own] + [hop(own, sizes, k, 0) for k in range(1, size_a)]
    step = size_b // 2
    while step > 1:
        direct = [hop(own, sizes, k, step) for k in range(min(2, size_a))] if len(blocks) == size_a else []
        blocks = blocks + direct + [hop(b, sizes, 0, step) for b in blocks[len(direct) :]]
        step //= 2
    ready = ((qk, val, out, hid, fin), (qk_b, val_b, out_b, hid_b, gain, shift, fin_b))
    half = len(blocks)
    arrays = blocks + ([hop(b, sizes, 0, 1) for b in blocks] if size_b > 1 else [])
    layers = qk.shape[0]
    for layer in range(layers - 1):
        (result,) = layer_call(arrays, half, rows_a, rows_b, ready, layer, False)
        arrays = [result] + ([hop(result, sizes, 0, 1)] if size_b > 1 else [])
    return tuple(layer_call(arrays, 1, rows_a, rows_b, ready, layers - 1, True))


def matmul(left, right):
    return jnp.dot(left, right, precision=EXACT_RESULT)


def layer_norm(values, gain, offset):
    average = jnp.mean(values, -1, keepdims=True)
    centred = values - average
    spread = jnp.mean(centred * centred, -1, keepdims=True)
    return centred / jnp.sqrt(spread + EPS) * gain + offset


def feed_forward_rows(state, message, hidden_weight, hidden_bias, norm_gain, norm_bias, final_weight, final_bias):
    joined = jnp.concatenate([state, message], -1)
    hidden = matmul(joined, hidden_weight) + hidden_bias
    active = jax.nn.gelu(layer_norm(hidden, norm_gain, norm_bias), approximate=False)
    return state + matmul(active, final_weight) + final_bias


def settle_owner(numer, tops, totals):
    best = jnp.max(tops, 0)
    weight = jnp.exp(tops - best[None])
    denom = jnp.sum(weight * totals, 0)
    sources = numer.shape[0]
    rows = numer.shape[1]
    heads = tops.shape[2]
    shaped = numer.reshape(sources, rows, heads, -1)
    joined = jnp.sum(shaped * weight[:, :, :, None], 0) / denom[:, :, None]
    return joined.reshape(rows, -1)


def partitioned(
    feats_a,
    feats_b,
    qk_weight,
    qk_bias,
    value_weight,
    value_bias,
    out_weight,
    out_bias,
    hidden_weight,
    hidden_bias,
    norm_gain,
    norm_bias,
    final_weight,
    final_bias,
):
    width = feats_a.shape[1]
    head_count = HEADS
    head_width = width // head_count
    softmax_temper = head_width ** (-0.5)
    first = feats_a
    second = feats_b

    def exchange(x, axis):
        return lax.all_to_all(x[None], axis, split_axis=1, concat_axis=0, tiled=True)

    for layer in range(qk_weight.shape[0]):
        joint_weight = jnp.concatenate([qk_weight[layer], value_weight[layer]], 1)
        joint_bias = jnp.concatenate([qk_bias[layer], value_bias[layer]], 0)
        proj_a = matmul(first, joint_weight) + joint_bias
        proj_b = matmul(second, joint_weight) + joint_bias
        block_a = lax.all_gather(proj_a, "ba", axis=0, tiled=True)
        block_b = lax.all_gather(proj_b, "aa", axis=0, tiled=True)
        query_a = block_a[:, :width].reshape(-1, head_count, head_width)
        value_a = block_a[:, width:].reshape(-1, head_count, head_width)
        query_b = block_b[:, :width].reshape(-1, head_count, head_width)
        value_b = block_b[:, width:].reshape(-1, head_count, head_width)
        scores = jnp.einsum("cjg,xjg->jcx", query_a, query_b, precision=EXACT_RESULT) * softmax_temper
        row_local = jnp.max(scores, 2)
        col_local = jnp.max(scores, 1)
        row_exp = jnp.exp(scores - row_local[:, :, None])
        col_exp = jnp.exp(scores - col_local[:, None, :])
        numer_a = jnp.einsum("hab,bhd->ahd", row_exp, value_b, precision=EXACT_RESULT).reshape(-1, width)
        numer_b = jnp.einsum("hab,ahd->bhd", col_exp, value_a, precision=EXACT_RESULT).reshape(-1, width)
        msg_a = settle_owner(
            exchange(numer_a, "ba"),
            exchange(jnp.transpose(row_local), "ba"),
            exchange(jnp.transpose(jnp.sum(row_exp, 2)), "ba"),
        )
        msg_b = settle_owner(
            exchange(numer_b, "aa"),
            exchange(jnp.transpose(col_local), "aa"),
            exchange(jnp.transpose(jnp.sum(col_exp, 1)), "aa"),
        )
        tail = (
            hidden_weight[layer],
            hidden_bias[layer],
            norm_gain[layer],
            norm_bias[layer],
            final_weight[layer],
            final_bias[layer],
        )
        first = feed_forward_rows(first, matmul(msg_a, out_weight[layer]) + out_bias[layer], *tail)
        second = feed_forward_rows(second, matmul(msg_b, out_weight[layer]) + out_bias[layer], *tail)
    return (first, second)


def shards(sizes, feats_a, feats_b, *weights):
    devices = sizes[0] * sizes[1]
    gathered = devices * (feats_a.size + feats_b.size) * feats_a.dtype.itemsize
    regular = all(n & (n - 1) == 0 for n in sizes) and feats_a.shape[0] % 8 == 0 and feats_b.shape[0] % 8 == 0
    if regular and gathered <= GATHER_BYTES:
        return replicated(sizes, feats_a, feats_b, *weights)
    return partitioned(feats_a, feats_b, *weights)


def solution(mesh):
    sizes = (mesh.shape["aa"], mesh.shape["ba"])
    in_specs = (P(("pairs", "aa", "ba"), None), P(("pairs", "ba", "aa"), None)) + (P(),) * 12
    out_specs = (P(("pairs", "aa", "ba"), None), P(("pairs", "ba", "aa"), None))
    return jax.shard_map(
        functools.partial(shards, sizes), mesh=mesh, in_specs=in_specs, out_specs=out_specs, check_vma=False
    )
```

```python
import functools

import jax
import jax.numpy as jnp
from jax import lax
from jax.experimental import pallas as pl
from jax.experimental.pallas import tpu as pltpu
from jax.sharding import PartitionSpec as P

HEADS = 4
EPS = 1e-05
LOG2_E = 1.4426950408889634
EXACT_RESULT = lax.Precision.HIGHEST
GATHER_BYTES = 2 << 20

LEAD = 4


def split(x):
    hi = x.astype(jnp.bfloat16)
    return hi, (x - hi.astype(jnp.float32)).astype(jnp.bfloat16)


def dot(a, b, transposed=False):
    contract = ((1,), (1 if transposed else 0,))
    return lax.dot_general(a, b, (contract, ((), ())), preferred_element_type=jnp.float32)


def dot3(a, b, transposed=False):
    return dot(a[0], b[0], transposed) + (dot(a[0], b[1], transposed) + dot(a[1], b[0], transposed))


def turned(x):
    tiles = []
    for t in range(0, x.shape[1], 128):
        tiles += [x[:, t + 64 : t + 128], x[:, t : t + 64]]
    return jnp.concatenate(tiles, 1)


def lower_lanes(rows):
    return lax.broadcasted_iota(jnp.int32, (rows, 128), 1) < 64


def tile(x, h):
    t = (h // 2) * 128
    return x[:, t : t + 128]


def pick(low, left, right, left_turned, right_turned, h):
    if h % 2 == 0:
        return jnp.where(low, tile(left, h), tile(right_turned, h))
    return jnp.where(low, tile(left_turned, h), tile(right, h))


class Halves:
    def __init__(self, x):
        self.hi, self.lo = split(x)
        self.hi_t, self.lo_t = turned(self.hi), turned(self.lo)

    def rows(self, rows):
        out = Halves.__new__(Halves)
        out.hi, out.lo, out.hi_t, out.lo_t = self.hi[rows], self.lo[rows], self.hi_t[rows], self.lo_t[rows]
        return out

    def query(self, h):
        low = lower_lanes(self.hi.shape[0])
        return jnp.concatenate(
            [pick(low, self.hi, self.hi, self.hi_t, self.hi_t, h), pick(low, self.lo, self.lo, self.lo_t, self.lo_t, h)], 1
        )

    def mixed(self, h):
        return pick(lower_lanes(self.hi.shape[0]), self.hi, self.lo, self.hi_t, self.lo_t, h)


def attend(query, keys, values, temper):
    def weigh(scores, value):
        weights = jnp.exp2((scores - jnp.max(scores, 1, keepdims=True)) * (temper * LOG2_E))
        hi, lo = split(weights)
        numer = dot(hi, value) + dot(lo, value)
        folded = numer[:, :128]
        folded = folded + pltpu.roll(folded, 64, 1)
        return folded * (1.0 / numer[:, 128:])

    heads = len(keys)
    ahead = dot(query(0), keys[0], True)
    yield
    results = []
    for h in range(heads):
        scores = ahead
        if h + 1 < heads:
            ahead = dot(query(h + 1), keys[h + 1], True)
            yield
        results.append(weigh(scores, values[h]))
        yield
    low = lower_lanes(results[0].shape[0])
    return jnp.concatenate([jnp.where(low, results[h], results[h + 1]) for h in range(0, heads, 2)], 1)


def interleave(first, second, lead):
    done = {}
    streams = [first, second]

    def step(i):
        try:
            next(streams[i])
        except StopIteration as stop:
            done[i] = stop.value

    for _ in range(lead):
        if 0 not in done:
            step(0)
    while len(done) < 2:
        for i in (1, 0):
            if i not in done:
                step(i)
    return done[0], done[1]


def anchor_kernel(x_ref, o_ref):
    del x_ref, o_ref


def anchor(x):
    vmem = pl.BlockSpec(memory_space=pltpu.VMEM)
    return pl.pallas_call(
        anchor_kernel,
        in_specs=[vmem],
        out_specs=vmem,
        out_shape=jax.ShapeDtypeStruct(x.shape, x.dtype),
        input_output_aliases={0: 0},
        cost_estimate=pl.CostEstimate(flops=10**10, bytes_accessed=1, transcendentals=0),
        compiler_params=pltpu.CompilerParams(vmem_limit_bytes=1 << 20),
        name="anchor",
    )(x)


def own_block(feats_a, feats_b):
    rows_a, rows_b = feats_a.shape[0], feats_b.shape[0]
    low = jnp.float32(-jnp.inf)
    padded_a = lax.pad(feats_a, low, [(0, rows_b, 0), (0, 0, 0)])
    padded_b = lax.pad(feats_b, low, [(rows_a, 0, 0), (0, 0, 0)])
    return jnp.maximum(padded_a, padded_b)


def layer_kernel(layer, spans, n_tgt, rows_a, rows_b, heads, *refs):
    srcs = refs[: len(spans)]
    rest = refs[len(spans) :]

    def mat(i):
        return split(rest[i][layer])

    def vec(i):
        return rest[5 + i][layer : layer + 1, :]

    qk_b, val_b, out_b, hid_b, gain, shift, fin_b = (vec(i) for i in range(7))
    outs = rest[12:]
    parts_a, parts_b = [], []
    for s, span in zip(srcs, spans):
        parts_a.append(s[: span * rows_a, :])
        parts_b.append(s[span * rows_a :, :])
    xs = jnp.concatenate(parts_a + parts_b, 0)
    width = xs.shape[1]
    temper = (width // heads) ** (-0.5)
    halves = split(xs)
    qk = dot3(halves, mat(0)) + qk_b
    val = dot3(halves, mat(1)) + val_b
    count_a = len(parts_a) * rows_a
    tgt_a, tgt_b = n_tgt * rows_a, n_tgt * rows_b
    qk_halves, val_halves = Halves(qk), Halves(val)
    keys = [jnp.concatenate([m, m], 1) for m in (qk_halves.mixed(h) for h in range(heads))]
    ones = jnp.ones((xs.shape[0], 128), jnp.bfloat16)
    values = [jnp.concatenate([val_halves.mixed(h), ones], 1) for h in range(heads)]
    rows_of = {0: slice(0, count_a), 1: slice(count_a, None)}
    out_w, hid, fin = mat(2), mat(3), mat(4)
    hid_x, hid_y = tuple(h[:width] for h in hid), tuple(h[width:] for h in hid)

    def stream(start, stop, side):
        q = qk_halves.rows(slice(start, stop))
        other = rows_of[1 - side]
        msg = yield from attend(q.query, [k[other] for k in keys], [v[other] for v in values], temper)
        x = xs[start:stop]
        y = dot3(split(msg), out_w) + out_b
        yield
        hidden = dot3(split(x), hid_x) + dot3(split(y), hid_y) + hid_b
        yield
        centred = hidden - jnp.mean(hidden, 1, keepdims=True)
        spread = jnp.mean(centred * centred, 1, keepdims=True)
        normed = centred * lax.rsqrt(spread + EPS) * gain + shift
        active = split(0.5 * normed * (1.0 + lax.erf(normed * (0.5**0.5))))
        yield
        return x + dot3(active, fin) + fin_b

    res = interleave(stream(0, tgt_a, 0), stream(count_a, count_a + tgt_b, 1), LEAD)
    outs[0][:tgt_a, :], outs[0][tgt_a:, :] = res


def vmem_call(kernel, args, shapes, name, grant, flops):
    vmem = pl.BlockSpec(memory_space=pltpu.VMEM)
    moved = sum(a.size * a.dtype.itemsize for a in args)
    return pl.pallas_call(
        kernel,
        in_specs=[vmem] * len(args),
        out_specs=[vmem] * len(shapes),
        out_shape=shapes,
        cost_estimate=pl.CostEstimate(flops=flops, bytes_accessed=moved, transcendentals=0),
        compiler_params=pltpu.CompilerParams(vmem_limit_bytes=grant),
        name=name,
    )(*args)


def layer_call(arrays, n_tgt, rows_a, rows_b, weights, layer):
    rows = rows_a + rows_b
    width = arrays[0].shape[1]
    spans = tuple(a.shape[0] // rows for a in arrays)
    return vmem_call(
        functools.partial(layer_kernel, layer, spans, n_tgt, rows_a, rows_b, HEADS),
        [*arrays, *weights[0], *weights[1]],
        [jax.ShapeDtypeStruct((n_tgt * rows, width), jnp.float32)],
        f"layer{layer}",
        24 << 20,
        12 * sum(spans) * rows * width * width,
    )[0]


def partial_softmax(u, shift, first, second, split_at):
    results = []
    for rows, source in ((slice(0, split_at), second), (slice(split_at, None), first)):
        x = split(source)
        scores = dot3(tuple(h[rows] for h in u), x, True) + shift[rows]
        top = jnp.max(scores, 1, keepdims=True)
        weights = jnp.exp(scores - top)
        results.append((top, jnp.sum(weights, 1, keepdims=True), dot3(split(weights), x)))
    return tuple(jnp.concatenate(pair, 0) for pair in zip(*results))


def head_masks(rows, width, heads):
    lane = lax.broadcasted_iota(jnp.int32, (rows, width), 1)
    size = width // heads
    return [(lane >= h * size) & (lane < (h + 1) * size) for h in range(heads)]


def stack_heads(x, masks):
    return jnp.concatenate([jnp.where(m, x, 0.0) for m in masks], 0)


def open_kernel(layer, rows_a, rows_b, heads, src, qk, qk_b, hid, hid_b, hi_ref, lo_ref, shift_ref, top_ref, sum_ref, numer_ref, hx_ref):
    width = src.shape[1]
    count_a = src.shape[0] * rows_a // (rows_a + rows_b)
    first, second = src[:count_a, :], src[count_a:, :]
    x = jnp.concatenate([first[:rows_a], second[:rows_b]], 0)
    halves, weight = split(x), split(qk[layer])
    bias = qk_b[layer : layer + 1, :]
    q = (dot3(halves, weight) + bias) * (width // heads) ** (-0.5)
    stacked = jnp.concatenate(
        [stack_heads(q[:rows_a], head_masks(rows_a, width, heads)), stack_heads(q[rows_a:], head_masks(rows_b, width, heads))], 0
    )
    shift = jnp.sum(stacked * bias, 1, keepdims=True)
    u = split(dot3(split(stacked), weight, True))
    hi_ref[...], lo_ref[...] = u
    top, total, numer = partial_softmax(u, shift, first, second, heads * rows_a)
    wide = shift_ref.shape
    shift_ref[...] = jnp.broadcast_to(shift, wide)
    top_ref[...] = jnp.broadcast_to(top, wide)
    sum_ref[...] = jnp.broadcast_to(total, wide)
    numer_ref[...] = numer
    hx_ref[...] = dot3(halves, split(hid[layer, :width, :])) + hid_b[layer : layer + 1, :]


def close_kernel(layer, rows_a, rows_b, heads, *refs):
    own, other, hi, lo, shift, top, total, numer, hx, val, val_b, out, out_b, hid, gain, scale_shift, fin, fin_b, out_a, out_b_ref = refs
    width = own.shape[1]
    tall = heads * rows_a

    def vec(r):
        return r[layer : layer + 1, :]

    top1, total1, numer1 = top[:, :1], total[:, :1], numer[...]
    if True:
        count_a = other.shape[0] * rows_a // (rows_a + rows_b)
        top2, total2, numer2 = partial_softmax((hi[...], lo[...]), shift[:, :1], other[:count_a, :], other[count_a:, :], tall)
        best = jnp.maximum(top1, top2)
        keep1, keep2 = jnp.exp(top1 - best), jnp.exp(top2 - best)
        numer1 = numer1 * keep1 + numer2 * keep2
        total1 = total1 * keep1 + total2 * keep2
    mixed_rows = dot3(split(numer1 * (1.0 / total1)), split(val[layer]))
    msgs = []
    for rows, begin in ((rows_a, 0), (rows_b, tall)):
        msg = jnp.zeros((rows, width), jnp.float32)
        for h, m in enumerate(head_masks(rows, width, heads)):
            msg = jnp.where(m, mixed_rows[begin + h * rows : begin + (h + 1) * rows], msg)
        msgs.append(msg)
    msg = jnp.concatenate(msgs, 0) + vec(val_b)
    y = dot3(split(msg), split(out[layer])) + vec(out_b)
    hidden = hx[...] + dot3(split(y), split(hid[layer, width:, :]))
    centred = hidden - jnp.mean(hidden, 1, keepdims=True)
    spread = jnp.mean(centred * centred, 1, keepdims=True)
    normed = centred * lax.rsqrt(spread + EPS) * vec(gain) + vec(scale_shift)
    active = 0.5 * normed * (1.0 + lax.erf(normed * (0.5**0.5)))
    count_own = own.shape[0] * rows_a // (rows_a + rows_b)
    x = jnp.concatenate([own[:rows_a, :], own[count_own : count_own + rows_b, :]], 0)
    res = x + dot3(split(active), split(fin[layer])) + vec(fin_b)
    out_a[...] = res[:rows_a]
    out_b_ref[...] = res[rows_a:]


def last_layer(own, other, rows_a, rows_b, mats, vecs, layer):
    qk, val, out, hid, fin = mats
    qk_b, val_b, out_b, hid_b, gain, shift, fin_b = vecs
    width = own.shape[1]
    rows = rows_a + rows_b
    tall = HEADS * rows
    f32 = lambda *s: jax.ShapeDtypeStruct(s, jnp.float32)
    half = jax.ShapeDtypeStruct((tall, width), jnp.bfloat16)
    state = vmem_call(
        functools.partial(open_kernel, layer, rows_a, rows_b, HEADS),
        [own, qk, qk_b, hid, hid_b],
        [half, half, f32(tall, 128), f32(tall, 128), f32(tall, 128), f32(tall, width), f32(rows, hid.shape[2])],
        "open_last",
        8 << 20,
        2 * tall * width * own.shape[0],
    )
    return vmem_call(
        functools.partial(close_kernel, layer, rows_a, rows_b, HEADS),
        [own, other, *state, val, val_b, out, out_b, hid, gain, shift, fin, fin_b],
        [f32(rows_a, width), f32(rows_b, width)],
        "close_last",
        12 << 20,
        2 * tall * width * own.shape[0],
    )


def hop(x, sizes, step_a, step_b):
    size_a, size_b = sizes
    pairs = [
        (a * size_b + b, (a ^ step_a) * size_b + (b ^ step_b)) for a in range(size_a) for b in range(size_b)
    ]
    return lax.ppermute(x, ("aa", "ba"), pairs)


def replicated(sizes, feats_a, feats_b, *weights):
    size_a, size_b = sizes
    rows_a, rows_b = feats_a.shape[0], feats_b.shape[0]
    qk, qk_b, val, val_b, out, out_b, hid, hid_b, gain, shift, fin, fin_b = weights
    own = anchor(own_block(feats_a, feats_b))
    blocks = [own] + [hop(own, sizes, k, 0) for k in range(1, size_a)]
    step = size_b // 2
    while step > 1:
        direct = [hop(own, sizes, k, step) for k in range(min(2, size_a))] if len(blocks) == size_a else []
        blocks = blocks + direct + [hop(b, sizes, 0, step) for b in blocks[len(direct) :]]
        step //= 2
    ready = ((qk, val, out, hid, fin), (qk_b, val_b, out_b, hid_b, gain, shift, fin_b))
    half = len(blocks)
    arrays = blocks + [hop(b, sizes, 0, 1) for b in blocks]
    layers = qk.shape[0]
    for layer in range(layers - 1):
        result = layer_call(arrays, half, rows_a, rows_b, ready, layer)
        arrays = [result, hop(result, sizes, 0, 1)]
    return tuple(last_layer(*arrays, rows_a, rows_b, *ready, layers - 1))


def matmul(left, right):
    return jnp.dot(left, right, precision=EXACT_RESULT)


def layer_norm(values, gain, offset):
    average = jnp.mean(values, -1, keepdims=True)
    centred = values - average
    spread = jnp.mean(centred * centred, -1, keepdims=True)
    return centred / jnp.sqrt(spread + EPS) * gain + offset


def feed_forward_rows(state, message, hidden_weight, hidden_bias, norm_gain, norm_bias, final_weight, final_bias):
    joined = jnp.concatenate([state, message], -1)
    hidden = matmul(joined, hidden_weight) + hidden_bias
    active = jax.nn.gelu(layer_norm(hidden, norm_gain, norm_bias), approximate=False)
    return state + matmul(active, final_weight) + final_bias


def settle_owner(numer, tops, totals):
    best = jnp.max(tops, 0)
    weight = jnp.exp(tops - best[None])
    denom = jnp.sum(weight * totals, 0)
    sources = numer.shape[0]
    rows = numer.shape[1]
    heads = tops.shape[2]
    shaped = numer.reshape(sources, rows, heads, -1)
    joined = jnp.sum(shaped * weight[:, :, :, None], 0) / denom[:, :, None]
    return joined.reshape(rows, -1)


def partitioned(
    feats_a,
    feats_b,
    qk_weight,
    qk_bias,
    value_weight,
    value_bias,
    out_weight,
    out_bias,
    hidden_weight,
    hidden_bias,
    norm_gain,
    norm_bias,
    final_weight,
    final_bias,
):
    width = feats_a.shape[1]
    head_count = HEADS
    head_width = width // head_count
    softmax_temper = head_width ** (-0.5)
    first = feats_a
    second = feats_b

    def exchange(x, axis):
        return lax.all_to_all(x[None], axis, split_axis=1, concat_axis=0, tiled=True)

    for layer in range(qk_weight.shape[0]):
        joint_weight = jnp.concatenate([qk_weight[layer], value_weight[layer]], 1)
        joint_bias = jnp.concatenate([qk_bias[layer], value_bias[layer]], 0)
        proj_a = matmul(first, joint_weight) + joint_bias
        proj_b = matmul(second, joint_weight) + joint_bias
        block_a = lax.all_gather(proj_a, "ba", axis=0, tiled=True)
        block_b = lax.all_gather(proj_b, "aa", axis=0, tiled=True)
        query_a = block_a[:, :width].reshape(-1, head_count, head_width)
        value_a = block_a[:, width:].reshape(-1, head_count, head_width)
        query_b = block_b[:, :width].reshape(-1, head_count, head_width)
        value_b = block_b[:, width:].reshape(-1, head_count, head_width)
        scores = jnp.einsum("cjg,xjg->jcx", query_a, query_b, precision=EXACT_RESULT) * softmax_temper
        row_local = jnp.max(scores, 2)
        col_local = jnp.max(scores, 1)
        row_exp = jnp.exp(scores - row_local[:, :, None])
        col_exp = jnp.exp(scores - col_local[:, None, :])
        numer_a = jnp.einsum("hab,bhd->ahd", row_exp, value_b, precision=EXACT_RESULT).reshape(-1, width)
        numer_b = jnp.einsum("hab,ahd->bhd", col_exp, value_a, precision=EXACT_RESULT).reshape(-1, width)
        msg_a = settle_owner(
            exchange(numer_a, "ba"),
            exchange(jnp.transpose(row_local), "ba"),
            exchange(jnp.transpose(jnp.sum(row_exp, 2)), "ba"),
        )
        msg_b = settle_owner(
            exchange(numer_b, "aa"),
            exchange(jnp.transpose(col_local), "aa"),
            exchange(jnp.transpose(jnp.sum(col_exp, 1)), "aa"),
        )
        tail = (
            hidden_weight[layer],
            hidden_bias[layer],
            norm_gain[layer],
            norm_bias[layer],
            final_weight[layer],
            final_bias[layer],
        )
        first = feed_forward_rows(first, matmul(msg_a, out_weight[layer]) + out_bias[layer], *tail)
        second = feed_forward_rows(second, matmul(msg_b, out_weight[layer]) + out_bias[layer], *tail)
    return (first, second)


def shards(sizes, feats_a, feats_b, *weights):
    devices = sizes[0] * sizes[1]
    gathered = devices * (feats_a.size + feats_b.size) * feats_a.dtype.itemsize
    regular = all(n & (n - 1) == 0 for n in sizes) and sizes[1] > 1 and weights[0].shape[0] > 1 and feats_a.shape[0] % 8 == 0 and feats_b.shape[0] % 8 == 0
    if regular and gathered <= GATHER_BYTES:
        return replicated(sizes, feats_a, feats_b, *weights)
    return partitioned(feats_a, feats_b, *weights)


def solution(mesh):
    sizes = (mesh.shape["aa"], mesh.shape["ba"])
    in_specs = (P(("pairs", "aa", "ba"), None), P(("pairs", "ba", "aa"), None)) + (P(),) * 12
    out_specs = (P(("pairs", "aa", "ba"), None), P(("pairs", "ba", "aa"), None))
    return jax.shard_map(
        functools.partial(shards, sizes), mesh=mesh, in_specs=in_specs, out_specs=out_specs, check_vma=False
    )
```

```python
import functools

import jax
import jax.numpy as jnp
from jax import lax
from jax.experimental import pallas as pl
from jax.experimental.pallas import tpu as pltpu
from jax.sharding import PartitionSpec as P

HEADS = 4
EPS = 1e-05
LOG2_E = 1.4426950408889634
EXACT_RESULT = lax.Precision.HIGHEST
GATHER_BYTES = 2 << 20

LEAD = 2
SPLIT = 1


def split(x):
    hi = x.astype(jnp.bfloat16)
    return hi, (x - hi.astype(jnp.float32)).astype(jnp.bfloat16)


def dot(a, b, transposed=False):
    contract = ((1,), (1 if transposed else 0,))
    return lax.dot_general(a, b, (contract, ((), ())), preferred_element_type=jnp.float32)


def dot3_low(a, b, transposed=False):
    rows = a[0].shape[0]
    both = dot(jnp.concatenate(a, 0), b[0], transposed)
    return both[:rows] + (both[rows:] + dot(a[0], b[1], transposed))


def dot3(a, b, transposed=False):
    return dot(a[0], b[0], transposed) + (dot(a[0], b[1], transposed) + dot(a[1], b[0], transposed))


def turned(x):
    tiles = []
    for t in range(0, x.shape[1], 128):
        tiles += [x[:, t + 64 : t + 128], x[:, t : t + 64]]
    return jnp.concatenate(tiles, 1)


def lower_lanes(rows):
    return lax.broadcasted_iota(jnp.int32, (rows, 128), 1) < 64


def tile(x, h):
    t = (h // 2) * 128
    return x[:, t : t + 128]


def pick(low, left, right, left_turned, right_turned, h):
    if h % 2 == 0:
        return jnp.where(low, tile(left, h), tile(right_turned, h))
    return jnp.where(low, tile(left_turned, h), tile(right, h))


class Halves:
    def __init__(self, x):
        self.hi, self.lo = split(x)
        self.hi_t, self.lo_t = turned(self.hi), turned(self.lo)

    def rows(self, rows):
        out = Halves.__new__(Halves)
        out.hi, out.lo, out.hi_t, out.lo_t = self.hi[rows], self.lo[rows], self.hi_t[rows], self.lo_t[rows]
        return out

    def query(self, h):
        low = lower_lanes(self.hi.shape[0])
        return jnp.concatenate(
            [pick(low, self.hi, self.hi, self.hi_t, self.hi_t, h), pick(low, self.lo, self.lo, self.lo_t, self.lo_t, h)], 1
        )

    def mixed(self, h):
        return pick(lower_lanes(self.hi.shape[0]), self.hi, self.lo, self.hi_t, self.lo_t, h)


def attend(query, keys, values, temper):
    def weigh(scores, value):
        weights = jnp.exp2((scores - jnp.max(scores, 1, keepdims=True)) * (temper * LOG2_E))
        hi, lo = split(weights)
        rows = scores.shape[0]
        both = dot(jnp.concatenate([hi, lo], 0), value)
        numer = both[:rows] + both[rows:]
        folded = numer[:, :128]
        folded = folded + pltpu.roll(folded, 64, 1)
        return folded * (1.0 / numer[:, 128:])

    heads = len(keys)
    ahead = dot(query(0), keys[0], True)
    yield
    results = []
    for h in range(heads):
        scores = ahead
        if h + 1 < heads:
            ahead = dot(query(h + 1), keys[h + 1], True)
            yield
        results.append(weigh(scores, values[h]))
        yield
    low = lower_lanes(results[0].shape[0])
    return jnp.concatenate([jnp.where(low, results[h], results[h + 1]) for h in range(0, heads, 2)], 1)


def interleave(streams, lead):
    done = {}
    turn = 0
    while len(done) < len(streams):
        for i in reversed(range(len(streams))):
            if i not in done and turn >= i * lead:
                try:
                    next(streams[i])
                except StopIteration as stop:
                    done[i] = stop.value
        turn += 1
    return [done[i] for i in range(len(streams))]


def anchor_kernel(x_ref, o_ref):
    del x_ref, o_ref


def anchor(x):
    vmem = pl.BlockSpec(memory_space=pltpu.VMEM)
    return pl.pallas_call(
        anchor_kernel,
        in_specs=[vmem],
        out_specs=vmem,
        out_shape=jax.ShapeDtypeStruct(x.shape, x.dtype),
        input_output_aliases={0: 0},
        cost_estimate=pl.CostEstimate(flops=10**10, bytes_accessed=1, transcendentals=0),
        compiler_params=pltpu.CompilerParams(vmem_limit_bytes=1 << 20),
        name="anchor",
    )(x)


def own_block(feats_a, feats_b):
    rows_a, rows_b = feats_a.shape[0], feats_b.shape[0]
    low = jnp.float32(-jnp.inf)
    padded_a = lax.pad(feats_a, low, [(0, rows_b, 0), (0, 0, 0)])
    padded_b = lax.pad(feats_b, low, [(rows_a, 0, 0), (0, 0, 0)])
    return jnp.maximum(padded_a, padded_b)


def layer_kernel(layer, spans, n_tgt, rows_a, rows_b, heads, *refs):
    srcs = refs[: len(spans)]
    rest = refs[len(spans) :]

    def mat(i):
        return split(rest[i][layer])

    def vec(i):
        return rest[5 + i][layer : layer + 1, :]

    qk_b, val_b, out_b, hid_b, gain, shift, fin_b = (vec(i) for i in range(7))
    outs = rest[12:]
    parts_a, parts_b = [], []
    for s, span in zip(srcs, spans):
        parts_a.append(s[: span * rows_a, :])
        parts_b.append(s[span * rows_a :, :])
    xs = jnp.concatenate(parts_a + parts_b, 0)
    width = xs.shape[1]
    temper = (width // heads) ** (-0.5)
    halves = split(xs)
    qk = dot3(halves, mat(0)) + qk_b
    val = dot3(halves, mat(1)) + val_b
    count_a = len(parts_a) * rows_a
    tgt_a, tgt_b = n_tgt * rows_a, n_tgt * rows_b
    qk_halves, val_halves = Halves(qk), Halves(val)
    keys = [jnp.concatenate([m, m], 1) for m in (qk_halves.mixed(h) for h in range(heads))]
    ones = jnp.ones((xs.shape[0], 128), jnp.bfloat16)
    values = [jnp.concatenate([val_halves.mixed(h), ones], 1) for h in range(heads)]
    rows_of = {0: slice(0, count_a), 1: slice(count_a, None)}
    out_w, hid, fin = mat(2), mat(3), mat(4)
    hid_x, hid_y = tuple(h[:width] for h in hid), tuple(h[width:] for h in hid)

    def stream(start, stop, side):
        q = qk_halves.rows(slice(start, stop))
        other = rows_of[1 - side]
        x = xs[start:stop]
        hidden_x = dot3(split(x), hid_x) + hid_b
        yield
        msg = yield from attend(q.query, [k[other] for k in keys], [v[other] for v in values], temper)
        y = dot3(split(msg), out_w) + out_b
        yield
        hidden = hidden_x + dot3(split(y), hid_y)
        yield
        centred = hidden - jnp.mean(hidden, 1, keepdims=True)
        spread = jnp.mean(centred * centred, 1, keepdims=True)
        normed = centred * lax.rsqrt(spread + EPS) * gain + shift
        active = split(0.5 * normed * (1.0 + lax.erf(normed * (0.5**0.5))))
        yield
        return x + dot3(active, fin) + fin_b

    cuts = [(i * tgt_a // SPLIT, (i + 1) * tgt_a // SPLIT, 0) for i in range(SPLIT)] + [(count_a, count_a + tgt_b, 1)]
    begin = 0
    for res in interleave([stream(*c) for c in cuts], LEAD):
        outs[0][begin : begin + res.shape[0], :] = res
        begin += res.shape[0]


def vmem_call(kernel, args, shapes, name, grant, flops, out_space=pltpu.VMEM, scratch=()):
    vmem = pl.BlockSpec(memory_space=pltpu.VMEM)
    moved = sum(a.size * a.dtype.itemsize for a in args)
    return pl.pallas_call(
        kernel,
        in_specs=[vmem] * len(args),
        out_specs=[pl.BlockSpec(memory_space=out_space)] * len(shapes),
        out_shape=shapes,
        scratch_shapes=scratch,
        cost_estimate=pl.CostEstimate(flops=flops, bytes_accessed=moved, transcendentals=0),
        compiler_params=pltpu.CompilerParams(vmem_limit_bytes=grant),
        name=name,
    )(*args)


def layer_call(arrays, n_tgt, rows_a, rows_b, weights, layer):
    rows = rows_a + rows_b
    width = arrays[0].shape[1]
    spans = tuple(a.shape[0] // rows for a in arrays)
    return vmem_call(
        functools.partial(layer_kernel, layer, spans, n_tgt, rows_a, rows_b, HEADS),
        [*arrays, *weights[0], *weights[1]],
        [jax.ShapeDtypeStruct((n_tgt * rows, width), jnp.float32)],
        f"layer{layer}",
        24 << 20,
        12 * sum(spans) * rows * width * width,
    )[0]


def partial_softmax(u, shift, first, second, split_at):
    results = []
    for rows, source in ((slice(0, split_at), second), (slice(split_at, None), first)):
        x = split(source)
        scores = dot3_low(tuple(h[rows] for h in u), x, True) + shift[rows]
        top = jnp.max(scores, 1, keepdims=True)
        weights = jnp.exp(scores - top)
        results.append((top, jnp.sum(weights, 1, keepdims=True), dot3_low(split(weights), x)))
    return tuple(jnp.concatenate(pair, 0) for pair in zip(*results))


def head_masks(rows, width, heads):
    lane = lax.broadcasted_iota(jnp.int32, (rows, width), 1)
    size = width // heads
    return [(lane >= h * size) & (lane < (h + 1) * size) for h in range(heads)]


def stack_heads(x, masks):
    return jnp.concatenate([jnp.where(m, x, 0.0) for m in masks], 0)


def open_kernel(layer, rows_a, rows_b, heads, src, qk, qk_b, hid, hid_b, hi_ref, lo_ref, shift_ref, top_ref, sum_ref, numer_ref, hx_ref):
    width = src.shape[1]
    count_a = src.shape[0] * rows_a // (rows_a + rows_b)
    first, second = src[:count_a, :], src[count_a:, :]
    x = jnp.concatenate([first[:rows_a], second[:rows_b]], 0)
    halves, weight = split(x), split(qk[layer])
    bias = qk_b[layer : layer + 1, :]
    q = (dot3_low(halves, weight) + bias) * (width // heads) ** (-0.5)
    stacked = jnp.concatenate(
        [stack_heads(q[:rows_a], head_masks(rows_a, width, heads)), stack_heads(q[rows_a:], head_masks(rows_b, width, heads))], 0
    )
    shift = jnp.sum(stacked * bias, 1, keepdims=True)
    u = split(dot3_low(split(stacked), weight, True))
    hi_ref[...], lo_ref[...] = u
    top, total, numer = partial_softmax(u, shift, first, second, heads * rows_a)
    wide = shift_ref.shape
    shift_ref[...] = jnp.broadcast_to(shift, wide)
    top_ref[...] = jnp.broadcast_to(top, wide)
    sum_ref[...] = jnp.broadcast_to(total, wide)
    numer_ref[...] = numer
    hx_ref[...] = dot3_low(halves, split(hid[layer, :width, :])) + hid_b[layer : layer + 1, :]


def close_kernel(layer, rows_a, rows_b, heads, *refs):
    own, other, hi, lo, shift, top, total, numer, hx, val, val_b, out, out_b, hid, gain, scale_shift, fin, fin_b, out_a, out_b_ref, stage, sems = refs
    width = own.shape[1]
    tall = heads * rows_a

    def vec(r):
        return r[layer : layer + 1, :]

    top1, total1, numer1 = top[:, :1], total[:, :1], numer[...]
    if True:
        count_a = other.shape[0] * rows_a // (rows_a + rows_b)
        top2, total2, numer2 = partial_softmax((hi[...], lo[...]), shift[:, :1], other[:count_a, :], other[count_a:, :], tall)
        best = jnp.maximum(top1, top2)
        keep1, keep2 = jnp.exp(top1 - best), jnp.exp(top2 - best)
        numer1 = numer1 * keep1 + numer2 * keep2
        total1 = total1 * keep1 + total2 * keep2
    mixed_rows = dot3_low(split(numer1 * (1.0 / total1)), split(val[layer]))
    msgs = []
    for rows, begin in ((rows_a, 0), (rows_b, tall)):
        msg = jnp.zeros((rows, width), jnp.float32)
        for h, m in enumerate(head_masks(rows, width, heads)):
            msg = jnp.where(m, mixed_rows[begin + h * rows : begin + (h + 1) * rows], msg)
        msgs.append(msg)
    msg = jnp.concatenate(msgs, 0) + vec(val_b)
    y = dot3_low(split(msg), split(out[layer])) + vec(out_b)
    hidden = hx[...] + dot3_low(split(y), split(hid[layer, width:, :]))
    centred = hidden - jnp.mean(hidden, 1, keepdims=True)
    spread = jnp.mean(centred * centred, 1, keepdims=True)
    normed = centred * lax.rsqrt(spread + EPS) * vec(gain) + vec(scale_shift)
    active = 0.5 * normed * (1.0 + lax.erf(normed * (0.5**0.5)))
    count_own = own.shape[0] * rows_a // (rows_a + rows_b)
    x = jnp.concatenate([own[:rows_a, :], own[count_own : count_own + rows_b, :]], 0)
    stage[...] = x + dot3_low(split(active), split(fin[layer])) + vec(fin_b)
    copies = [
        pltpu.make_async_copy(stage.at[:rows_a], out_a, sems.at[0]),
        pltpu.make_async_copy(stage.at[rows_a:], out_b_ref, sems.at[1]),
    ]
    for c in copies:
        c.start()
    for c in copies:
        c.wait()


def last_layer(own, other, rows_a, rows_b, mats, vecs, layer):
    qk, val, out, hid, fin = mats
    qk_b, val_b, out_b, hid_b, gain, shift, fin_b = vecs
    width = own.shape[1]
    rows = rows_a + rows_b
    tall = HEADS * rows
    f32 = lambda *s: jax.ShapeDtypeStruct(s, jnp.float32)
    half = jax.ShapeDtypeStruct((tall, width), jnp.bfloat16)
    state = vmem_call(
        functools.partial(open_kernel, layer, rows_a, rows_b, HEADS),
        [own, qk, qk_b, hid, hid_b],
        [half, half, f32(tall, 128), f32(tall, 128), f32(tall, 128), f32(tall, width), f32(rows, hid.shape[2])],
        "open_last",
        8 << 20,
        2 * tall * width * own.shape[0],
    )
    return vmem_call(
        functools.partial(close_kernel, layer, rows_a, rows_b, HEADS),
        [own, other, *state, val, val_b, out, out_b, hid, gain, shift, fin, fin_b],
        [f32(rows_a, width), f32(rows_b, width)],
        "close_last",
        12 << 20,
        2 * tall * width * own.shape[0],
        pltpu.HBM,
        [pltpu.VMEM((rows, width), jnp.float32), pltpu.SemaphoreType.DMA((2,))],
    )


def hop(x, sizes, step_a, step_b):
    size_a, size_b = sizes
    pairs = [
        (a * size_b + b, (a ^ step_a) * size_b + (b ^ step_b)) for a in range(size_a) for b in range(size_b)
    ]
    return lax.ppermute(x, ("aa", "ba"), pairs)


def replicated(sizes, feats_a, feats_b, *weights):
    size_a, size_b = sizes
    rows_a, rows_b = feats_a.shape[0], feats_b.shape[0]
    qk, qk_b, val, val_b, out, out_b, hid, hid_b, gain, shift, fin, fin_b = weights
    own = anchor(own_block(feats_a, feats_b))
    blocks = [own] + [hop(own, sizes, k, 0) for k in range(1, size_a)]
    step = size_b // 2
    while step > 1:
        direct = [hop(own, sizes, k, step) for k in range(min(2, size_a))] if len(blocks) == size_a else []
        blocks = blocks + direct + [hop(b, sizes, 0, step) for b in blocks[len(direct) :]]
        step //= 2
    ready = ((qk, val, out, hid, fin), (qk_b, val_b, out_b, hid_b, gain, shift, fin_b))
    half = len(blocks)
    arrays = blocks + [hop(b, sizes, 0, 1) for b in blocks]
    layers = qk.shape[0]
    for layer in range(layers - 1):
        result = layer_call(arrays, half, rows_a, rows_b, ready, layer)
        arrays = [result, hop(result, sizes, 0, 1)]
    return tuple(last_layer(*arrays, rows_a, rows_b, *ready, layers - 1))


def matmul(left, right):
    return jnp.dot(left, right, precision=EXACT_RESULT)


def layer_norm(values, gain, offset):
    average = jnp.mean(values, -1, keepdims=True)
    centred = values - average
    spread = jnp.mean(centred * centred, -1, keepdims=True)
    return centred / jnp.sqrt(spread + EPS) * gain + offset


def feed_forward_rows(state, message, hidden_weight, hidden_bias, norm_gain, norm_bias, final_weight, final_bias):
    joined = jnp.concatenate([state, message], -1)
    hidden = matmul(joined, hidden_weight) + hidden_bias
    active = jax.nn.gelu(layer_norm(hidden, norm_gain, norm_bias), approximate=False)
    return state + matmul(active, final_weight) + final_bias


def settle_owner(numer, tops, totals):
    best = jnp.max(tops, 0)
    weight = jnp.exp(tops - best[None])
    denom = jnp.sum(weight * totals, 0)
    sources = numer.shape[0]
    rows = numer.shape[1]
    heads = tops.shape[2]
    shaped = numer.reshape(sources, rows, heads, -1)
    joined = jnp.sum(shaped * weight[:, :, :, None], 0) / denom[:, :, None]
    return joined.reshape(rows, -1)


def partitioned(
    feats_a,
    feats_b,
    qk_weight,
    qk_bias,
    value_weight,
    value_bias,
    out_weight,
    out_bias,
    hidden_weight,
    hidden_bias,
    norm_gain,
    norm_bias,
    final_weight,
    final_bias,
):
    width = feats_a.shape[1]
    head_count = HEADS
    head_width = width // head_count
    softmax_temper = head_width ** (-0.5)
    first = feats_a
    second = feats_b

    def exchange(x, axis):
        return lax.all_to_all(x[None], axis, split_axis=1, concat_axis=0, tiled=True)

    for layer in range(qk_weight.shape[0]):
        joint_weight = jnp.concatenate([qk_weight[layer], value_weight[layer]], 1)
        joint_bias = jnp.concatenate([qk_bias[layer], value_bias[layer]], 0)
        proj_a = matmul(first, joint_weight) + joint_bias
        proj_b = matmul(second, joint_weight) + joint_bias
        block_a = lax.all_gather(proj_a, "ba", axis=0, tiled=True)
        block_b = lax.all_gather(proj_b, "aa", axis=0, tiled=True)
        query_a = block_a[:, :width].reshape(-1, head_count, head_width)
        value_a = block_a[:, width:].reshape(-1, head_count, head_width)
        query_b = block_b[:, :width].reshape(-1, head_count, head_width)
        value_b = block_b[:, width:].reshape(-1, head_count, head_width)
        scores = jnp.einsum("cjg,xjg->jcx", query_a, query_b, precision=EXACT_RESULT) * softmax_temper
        row_local = jnp.max(scores, 2)
        col_local = jnp.max(scores, 1)
        row_exp = jnp.exp(scores - row_local[:, :, None])
        col_exp = jnp.exp(scores - col_local[:, None, :])
        numer_a = jnp.einsum("hab,bhd->ahd", row_exp, value_b, precision=EXACT_RESULT).reshape(-1, width)
        numer_b = jnp.einsum("hab,ahd->bhd", col_exp, value_a, precision=EXACT_RESULT).reshape(-1, width)
        msg_a = settle_owner(
            exchange(numer_a, "ba"),
            exchange(jnp.transpose(row_local), "ba"),
            exchange(jnp.transpose(jnp.sum(row_exp, 2)), "ba"),
        )
        msg_b = settle_owner(
            exchange(numer_b, "aa"),
            exchange(jnp.transpose(col_local), "aa"),
            exchange(jnp.transpose(jnp.sum(col_exp, 1)), "aa"),
        )
        tail = (
            hidden_weight[layer],
            hidden_bias[layer],
            norm_gain[layer],
            norm_bias[layer],
            final_weight[layer],
            final_bias[layer],
        )
        first = feed_forward_rows(first, matmul(msg_a, out_weight[layer]) + out_bias[layer], *tail)
        second = feed_forward_rows(second, matmul(msg_b, out_weight[layer]) + out_bias[layer], *tail)
    return (first, second)


def shards(sizes, feats_a, feats_b, *weights):
    devices = sizes[0] * sizes[1]
    gathered = devices * (feats_a.size + feats_b.size) * feats_a.dtype.itemsize
    regular = all(n & (n - 1) == 0 for n in sizes) and sizes[1] > 1 and weights[0].shape[0] > 1 and feats_a.shape[0] % 8 == 0 and feats_b.shape[0] % 8 == 0
    if regular and gathered <= GATHER_BYTES:
        return replicated(sizes, feats_a, feats_b, *weights)
    return partitioned(feats_a, feats_b, *weights)


def solution(mesh):
    sizes = (mesh.shape["aa"], mesh.shape["ba"])
    in_specs = (P(("pairs", "aa", "ba"), None), P(("pairs", "ba", "aa"), None)) + (P(),) * 12
    out_specs = (P(("pairs", "aa", "ba"), None), P(("pairs", "ba", "aa"), None))
    return jax.shard_map(
        functools.partial(shards, sizes), mesh=mesh, in_specs=in_specs, out_specs=out_specs, check_vma=False
    )
```
